512 devices in a mesh: grp: 2 (over y), chan: 32 (over z), col: 4 (over x), sub: 2 (over core).
Axes of the slice: x: 4, y: 2, z: 32, core: 2. Of those that a mesh axis runs over, the one named last changes fastest.
The devices are a block of a 4x16x32 slice.
Arguments:
- generator: float32 [64, 1024, 1024], P(('grp', 'chan'), 'sub', 'col'), parts along dimension 0, may hold values from -2 to 2
- interaction: float32 [64, 1024, 1024], P(('grp', 'chan'), 'sub', 'col'), parts along dimension 0, may hold values from -2 to 2
- occupations: int32 [160], replicated, may hold values 0 or 1
- pair_orbits: int32 [32, 2, 1024], P('chan'), may hold values from 0 to 159
- cross_orbits: int32 [32, 2, 1024], P('chan'), may hold values from 0 to 159
- pair_sizes: int32 [32], P('chan'), may hold values from 256 to 1024
- cross_sizes: int32 [32], P('chan'), may hold values from 256 to 1024
- cross_target: int32 [32, 32, 8], P('chan', 'sub', 'col'), may hold values from 0 to 1023, as said below
Outputs:
- commutator: float32 [64, 1024, 1024], P(('grp', 'chan'), 'sub', 'col'), parts along dimension 0
The draws below stay inside these ranges and needn't reach their ends.
There are 2 independent parts, one for each index of `grp`. The reference program is written for one: setup_inputs(seed, part) draws one part's arguments, and reference() takes and returns one part's arrays. A program takes and returns all parts, laid end to end along the dimension named above; an argument that names none is the same for every part. Nothing has to cross between parts.
Inputs may be any that keep to these rules, and one draw needn't show every extreme that they name: `cross_target`: each value is d * 32 + j: the tile goes to crossed channel d as tile j of the block with the same rows and columns as its own (tiles numbered row by row within the block). Every tile of every crossed channel receives exactly one tile. At most 2 tiles of one block go to one crossed channel, and in every block some crossed channel receives exactly 2.
All inputs are finite; a program needn't handle non-finite values.
Results may differ from the reference program's by a relative error of at most 0.0003.
Values sent between devices are 32-bit elements; how exact they have to be, the bound alone decides.
No kernel may reach another device: no remote copies, remote signals or barrier semaphores. Data moves between devices by JAX's collectives and lax.ppermute only.
A program may use at most 64 MiB of HBM per device.

```python
import jax
import jax.numpy as jnp
from jax import lax

ORBITALS = 160
M = 1024
TR = 32
TC = 128
CHANNELS = 32
TILES_DEV = 32
CAP = 2
N_COL = 4
N_SUB = 2


def shuffle_slots(slot_key):
    return jax.random.permutation(slot_key, TILES_DEV).astype(jnp.int32)


def one_block(key, block_index):
    block_key = jax.random.fold_in(key, block_index + 11)
    first_key, order_key, sender_key, taker_key = jax.random.split(block_key, 4)
    fullest = jax.random.randint(first_key, (), 0, CHANNELS)
    offsets = jnp.tile(jnp.arange(CHANNELS, dtype=jnp.int32), CAP)
    ranking = jax.random.permutation(order_key, CHANNELS * CAP).astype(jnp.int32)
    ranking = jnp.where(offsets == fullest, ranking - CHANNELS * CAP, ranking)
    shifts = offsets[jnp.argsort(ranking, stable=True)][:TILES_DEV]
    senders = jax.vmap(shuffle_slots)(jax.random.split(sender_key, CHANNELS))
    takers = jax.vmap(shuffle_slots)(jax.random.split(taker_key, CHANNELS))
    sources = jnp.arange(CHANNELS, dtype=jnp.int32)[:, None]
    owners = (sources + shifts[None, :]) % CHANNELS
    taken = takers[owners, jnp.arange(TILES_DEV, dtype=jnp.int32)[None, :]]
    values = owners * TILES_DEV + taken
    return jnp.take_along_axis(values, jnp.argsort(senders, axis=1, stable=True), axis=1)


def partial_block(key):

    def single_block(block_index):
        return one_block(key, block_index)
    return single_block


def draw_cross_target(key, part):
    block_rows = M // N_SUB // TR
    block_cols = M // N_COL // TC
    indices = jnp.arange(N_SUB * N_COL, dtype=jnp.int32)
    blocks = jax.vmap(partial_block(key))(indices)
    shaped = blocks.reshape(N_SUB, N_COL, CHANNELS, block_rows, block_cols)
    return shaped.transpose(2, 0, 3, 1, 4).reshape(CHANNELS, M // TR, M // TC).astype(jnp.int32)


def plant(values, own_key, least, largest):
    shape = values.shape
    index_at = [jax.random.randint(jax.random.fold_in(own_key, axis), (), 0, shape[axis]) for axis in range(len(shape))]
    values = values.at[tuple(index_at)].set(least)
    longest = shape.index(max(shape))
    index_at[longest] = (index_at[longest] + 1) % shape[longest]
    return values.at[tuple(index_at)].set(largest)


def block_scale(rng, extent, pieces, low, top_value):
    factor_of, own = 1.0, jax.random.fold_in(rng, 6)
    for axis_at, parts in pieces:
        draws = jnp.exp(jax.random.uniform(jax.random.fold_in(own, axis_at), (parts,), jnp.float32, low / len(pieces), top_value / len(pieces)))
        factor_of = factor_of * jnp.repeat(draws, extent[axis_at] // parts).reshape([-1 if axis == axis_at else 1 for axis in range(len(extent))])
    return factor_of


def gaussian(key, extent, width, bound, pieces=(), kind=jnp.bfloat16):
    loudness = block_scale(key, extent, pieces, -0.22, 0.18) if pieces else 1.0
    result = jax.random.normal(key, extent, jnp.float32) * width * loudness
    return jnp.minimum(jnp.maximum(result, -bound), bound).astype(kind)


def setup_inputs(seed: int = 0, part: int = 0) -> dict:
    streams_of = jax.random.split(jax.random.key(seed), 9)
    part_keys = jax.random.split(jax.random.fold_in(streams_of[8], part), 9)
    generator = gaussian(part_keys[0], (CHANNELS, M, M), 0.14, 2.0, ((0, 32), (1, 2), (2, 4)), jnp.float32)
    interaction = gaussian(part_keys[1], (CHANNELS, M, M), 0.14, 2.0, ((0, 32), (1, 2), (2, 4)), jnp.float32)
    occupations = plant((jax.random.randint(streams_of[2], (ORBITALS,), 0, 4) < 1).astype(jnp.int32), jax.random.fold_in(streams_of[2], 1), 0, 1)
    pair_orbits = plant(jax.random.randint(streams_of[3], (CHANNELS, 2, M), 0, ORBITALS), jax.random.fold_in(streams_of[3], 1), 0, ORBITALS - 1).astype(jnp.int32)
    cross_orbits = plant(jax.random.randint(streams_of[4], (CHANNELS, 2, M), 0, ORBITALS), jax.random.fold_in(streams_of[4], 1), 0, ORBITALS - 1).astype(jnp.int32)
    pair_sizes = plant(jax.random.randint(streams_of[5], (CHANNELS,), M // 4, M + 1), jax.random.fold_in(streams_of[5], 1), M // 4, M).astype(jnp.int32)
    cross_sizes = plant(jax.random.randint(streams_of[6], (CHANNELS,), M // 4, M + 1), jax.random.fold_in(streams_of[6], 1), M // 4, M).astype(jnp.int32)
    cross_target = draw_cross_target(jax.random.fold_in(streams_of[8], 71), part)
    return {"generator": generator, "interaction": interaction, "occupations": occupations, "pair_orbits": pair_orbits, "cross_orbits": cross_orbits, "pair_sizes": pair_sizes, "cross_sizes": cross_sizes, "cross_target": cross_target}


def occupancy(orbit_pairs, filled, size_limits, particle):
    first_filled = filled[orbit_pairs[:, 0, :]]
    second_filled = filled[orbit_pairs[:, 1, :]]
    live_pairs = (jnp.arange(M, dtype=jnp.int32)[None, :] < size_limits[:, None]).astype(jnp.float32)
    if particle:
        factor = 1.0 - first_filled - second_filled
    else:
        factor = first_filled - second_filled
    return factor * live_pairs


def bracket(left_side, right_side, weights):
    def single(operands):
        left_block, right_block, weight_row = operands
        forward = jnp.dot(left_block * weight_row[None, :], right_block, precision=lax.Precision.HIGHEST, preferred_element_type=jnp.float32)
        reverse = jnp.dot(right_block * weight_row[None, :], left_block, precision=lax.Precision.HIGHEST, preferred_element_type=jnp.float32)
        return forward - reverse
    return lax.map(single, (left_side, right_side, weights))


def split_tiles(matrices):
    channel_count = matrices.shape[0]
    tiled = matrices.reshape(channel_count, M // TR, TR, M // TC, TC)
    return tiled.transpose(0, 1, 3, 2, 4).reshape(-1, TR, TC)


def join_tiles(tiles, channel_count):
    tiled = tiles.reshape(channel_count, M // TR, M // TC, TR, TC)
    return tiled.transpose(0, 1, 3, 2, 4).reshape(channel_count, M, M)


def destinations(cross_target):
    block_rows = M // N_SUB // TR
    block_cols = M // N_COL // TC
    per_block = block_rows * block_cols
    channel_to = cross_target // per_block
    slot_to = cross_target % per_block
    tile_row = jnp.arange(M // TR, dtype=jnp.int32)[None, :, None]
    tile_col = jnp.arange(M // TC, dtype=jnp.int32)[None, None, :]
    row_to = (tile_row // block_rows) * block_rows + slot_to // block_cols
    col_to = (tile_col // block_cols) * block_cols + slot_to % block_cols
    return ((channel_to * (M // TR) + row_to) * (M // TC) + col_to).reshape(-1).astype(jnp.int32)


def reference(generator, interaction, occupations, pair_orbits, cross_orbits, pair_sizes, cross_sizes, cross_target):
    channel_count = generator.shape[0]
    filled = occupations.astype(jnp.float32)
    live_rows = (jnp.arange(M, dtype=jnp.int32)[None, :] < pair_sizes[:, None]).astype(jnp.float32)
    live_block = live_rows[:, :, None] * live_rows[:, None, :]
    generator_live = generator * live_block
    interaction_live = interaction * live_block
    particle = bracket(generator_live, interaction_live, occupancy(pair_orbits, filled, pair_sizes, True))
    flat_to = destinations(cross_target)
    empty_tiles = jnp.zeros((channel_count * (M // TR) * (M // TC), TR, TC), jnp.float32)
    crossed_generator = join_tiles(empty_tiles.at[flat_to].set(split_tiles(generator_live)), channel_count)
    crossed_interaction = join_tiles(empty_tiles.at[flat_to].set(split_tiles(interaction_live)), channel_count)
    crossed = bracket(crossed_generator, crossed_interaction, occupancy(cross_orbits, filled, cross_sizes, False))
    returned = join_tiles(split_tiles(crossed)[flat_to], channel_count)
    return live_block * (particle - returned)
```

```python
import functools

import jax
import jax.numpy as jnp
from jax import lax
from jax.experimental import pallas as pl
from jax.experimental.pallas import tpu as pltpu
from jax.sharding import PartitionSpec as P

TR = 32
TC = 128
FWD = ((0, 16), (16, 32))
RET = ((0, 16), (16, 32))
BF = jnp.bfloat16
F32 = jnp.float32


def smem():
    return pl.BlockSpec(memory_space=pltpu.SMEM)


def vmem():
    return pl.BlockSpec(memory_space=pltpu.VMEM)


def call(kernel, out_shape, args, n_smem, scratch=()):
    flat_out = jax.tree.leaves(out_shape)
    return pl.pallas_call(
        kernel,
        out_shape=out_shape,
        in_specs=[smem()] * n_smem + [vmem()] * (len(args) - n_smem),
        out_specs=jax.tree.unflatten(jax.tree.structure(out_shape), [vmem()] * len(flat_out)),
        scratch_shapes=list(scratch),
        compiler_params=pltpu.CompilerParams(vmem_limit_bytes=48 * 1024 * 1024),
    )(*args)


def f32(*shape):
    return jax.ShapeDtypeStruct(shape, F32)


def slot_rows(far, m, arr):
    return (2 * far + (1 if arr % 2 else 0)) * m


def id_rows(far, arr):
    return 2 * far + (8 if arr % 2 else 0)


def pack_kernel(far, slabs, codes, targets, meta, g_ref, h_ref, live_ref, *outs):
    rows = g_ref.shape[0]
    breadth = g_ref.shape[1] // TC
    size = meta[0]
    row0 = meta[1]
    col0 = meta[2]
    tiles = rows // TR * breadth
    for arr in range(4):
        base = slot_rows(far, slabs[0][1] - slabs[0][0], arr) * 2
        n = id_rows(far, arr)
        outs[arr][pl.ds(base, n), :] = jnp.full((n, TC), -1.0, F32)

    def body(r, carry):
        for t in range(breadth):
            i = r * breadth + t
            code = codes[i]
            arr_at = code // 32
            place = code % 32
            slot = lax.rem(targets[i], tiles).astype(F32)
            at = pl.multiple_of(r * TR, TR)
            live = ((lax.broadcasted_iota(jnp.int32, (TR, TC), 0) + row0 + r * TR) < size) & (
                (lax.broadcasted_iota(jnp.int32, (TR, TC), 1) + col0 + t * TC) < size
            )
            g = jnp.where(live, g_ref[pl.ds(at, TR), t * TC : (t + 1) * TC], 0.0)
            h = jnp.where(live, h_ref[pl.ds(at, TR), t * TC : (t + 1) * TC], 0.0)
            live_ref[0, t, pl.ds(at, TR), :] = g
            live_ref[1, t, pl.ds(at, TR), :] = h
            for arr in range(4):

                @pl.when(arr_at == arr)
                def _(arr=arr, g=g, h=h, slot=slot, place=place):
                    for s, (a, b) in enumerate(slabs):
                        m = b - a
                        ref = outs[4 * s + arr]
                        to = pl.multiple_of(place * (2 * m), 8)
                        ref[pl.ds(to, m), :] = g[a:b]
                        ref[pl.ds(to + m, m), :] = h[a:b]
                        if s == 0:
                            ref[pl.ds(slot_rows(far, 2 * m, arr) + place, 1), :] = jnp.full(
                                (1, TC), slot, F32
                            )

        return carry

    lax.fori_loop(0, rows // TR, body, 0)


def send(x, axis, hop, n):
    return lax.ppermute(x, axis, [(i, (i + hop) % n) for i in range(n)])


def repack_kernel(copies, *refs):
    out = refs[-1]
    for index, begin, end, to in copies:
        out[to : to + end - begin, :] = refs[index][begin:end, :]


def repack(arrays, copies, rows):
    used = sorted({c[0] for c in copies})
    copies = tuple((used.index(i), b, e, t) for i, b, e, t in copies)
    return call(
        functools.partial(repack_kernel, copies), f32(rows, TC), [arrays[i] for i in used], 0
    )


class Stream:
    def __init__(self, near, away, m, far, ids):
        self.m, self.far, self.ids = m, far, ids
        self.arrays = [near]
        self.where = {(d, e): (0, (2 * d + e) * m, 2 * far * m + 2 * d + e) for d in range(far) for e in range(2)}
        self.away = away

    def add(self, array, slots):
        self.arrays.append(array)
        m = self.m
        for k, slot in enumerate(slots):
            self.where[slot] = (len(self.arrays) - 1, k * m, len(slots) * m + k)

    def move(self, slots, hop, axis, n):
        m = self.m
        copies = []
        for k, slot in enumerate(slots):
            index, row, id_row = self.where[slot]
            for begin, end, to in [(row, row + m, k * m)] + (
                [(id_row, id_row + 1, len(slots) * m + k)] if self.ids else []
            ):
                copies.append((index, begin, end, to))
        merged = []
        for c in sorted(copies, key=lambda c: c[3]):
            if merged and merged[-1][0] == c[0] and merged[-1][2] == c[1]:
                merged[-1] = (c[0], merged[-1][1], c[2], merged[-1][3])
            else:
                merged.append(c)
        rows = len(slots) * m + (-(-len(slots) // 8) * 8 if self.ids else 0)
        self.add(send(repack(self.arrays, merged, rows), axis, hop, n), slots)

    def phase(self, hop, sign, axis, n):
        far = self.far
        if hop == far:
            slots = [(d, e) for d in range(far, 2 * far) for e in range(2)] + ["half"]
            self.add(send(self.away, axis, sign * hop, n), slots)
        else:
            slots = [(d, e) for d in range(2 * far) if d & hop for e in range(2)]
            slots.sort(key=lambda k: self.where[k])
            self.move(slots + ["half"], sign * hop, axis, n)

    def places(self):
        far = self.far
        found = [
            ((32 if d >= far else 0) + 2 * (d % far) + e, *self.where[d, e])
            for d in range(2 * far)
            for e in range(2)
        ]
        return found + [(32 + 2 * far, *self.where["half"])]


def transport(groups, widths, far, axis, n, sign, with_ids, between=None):
    streams = []
    for s, (a0, a1, a2, a3) in enumerate(groups):
        ids = with_ids and s == 0
        streams.append(
            (Stream(a0, a1, widths[s], far, ids), Stream(a2, a3, widths[s], far, ids))
        )
    hop = far
    while hop:
        for right, left in streams:
            right.phase(hop, sign, axis, n)
            left.phase(hop, -sign, axis, n)
        if hop == far:
            for right, left in streams:
                right.move(["half"], sign, axis, n)
                left.move(["half"], -sign, axis, n)
        if hop == 2 and between is not None:
            right = streams[0][0]
            right.arrays[-1], between = lax.optimization_barrier((right.arrays[-1], between))
        hop //= 2
    return streams, between


def ids_kernel(entries, *refs):
    ins, out, scratch = refs[:-2], refs[-2], refs[-1]
    scratch[...] = jnp.full(scratch.shape, -1.0, F32)
    for code, index, row in entries:
        scratch[code : code + 1, :] = ins[index][row : row + 1, :]
    shape = scratch.shape
    diagonal = lax.broadcasted_iota(jnp.int32, shape, 0) == lax.broadcasted_iota(jnp.int32, shape, 1)
    out[...] = jnp.sum(jnp.where(diagonal, scratch[...], 0.0), axis=0, keepdims=True).astype(jnp.int32)


def place_kernel(plan, slabs, ret, breadth, ids, *refs):
    n_in = sum(len(p[1]) for p in plan)
    ins, outs = refs[:n_in], refs[n_in:]
    block, pieces = outs[0], outs[1:]
    for s, first, entries in [(p[0], p[2], p[3]) for p in plan]:
        a, b = slabs[s]
        m = b - a
        for code, index, row in entries:
            slot = ids[code]

            @pl.when(slot >= 0)
            def _(slot=slot, index=index, row=row, first=first, a=a, m=m):
                r = slot // breadth
                t = slot % breadth
                ref = ins[first + index]
                for mat in range(2):
                    data = ref[row + mat * m : row + (mat + 1) * m, :]
                    block[mat, t, pl.ds(pl.multiple_of(r * TR + a, 8), m), :] = data
                    for q, (c, d) in enumerate(ret):
                        lo, hi = max(a, c), min(a + m, d)
                        if lo < hi:
                            pieces[q][
                                mat, t, pl.ds(pl.multiple_of(r * (d - c) + (lo - c), 8), hi - lo), :
                            ] = data[lo - a : hi - a]


def halves(x):
    high = x.astype(BF)
    return high, (x - high.astype(F32)).astype(BF)


def panel_kernel(meta, own, other, w_ref, high, low):
    rows = own.shape[2]
    breadth = own.shape[1]
    mine = pl.multiple_of(meta[3] * rows, rows)
    theirs = pl.multiple_of((1 - meta[3]) * rows, rows)
    step = 128
    for src, base in ((own, mine), (other, theirs)):
        for k in range(0, rows, step):
            at = pl.ds(pl.multiple_of(base + k, step), step)
            w = w_ref[at, :]
            for mat in range(2):
                for t in range(breadth):
                    x = src[1 - mat, t, k : k + step, :] * w
                    if mat == 1:
                        x = -x
                    hi, lo = halves(x)
                    high[mat, at, t * TC : (t + 1) * TC] = hi
                    low[mat, at, t * TC : (t + 1) * TC] = lo


def products(meta, pieces, high, low, out, n_col):
    rows = pieces[0].shape[2]
    breadth = pieces[0].shape[1]
    width = breadth * TC
    step = 128
    for c in range(0, rows, step):
        acc = jnp.zeros((step, width), F32)
        for d in range(n_col):
            at = pl.ds(pl.multiple_of(lax.rem(meta[4] + n_col - d, n_col) * width, width), width)
            for mat in range(2):
                x = jnp.concatenate([pieces[d][mat, t, c : c + step, :] for t in range(breadth)], 1)
                hi, lo = halves(x)
                bh = high[mat, at, :]
                bl = low[mat, at, :]
                acc += jnp.dot(hi, bh, preferred_element_type=F32)
                acc += jnp.dot(hi, bl, preferred_element_type=F32)
                acc += jnp.dot(lo, bh, preferred_element_type=F32)
        for t in range(breadth):
            out[t, c : c + step, :] = acc[:, t * TC : (t + 1) * TC]


def product_kernel(n_col, meta, *refs):
    pieces, (high, low, out) = refs[:n_col], refs[n_col:]
    products(meta, pieces, high, low, out, n_col)


def product_pick_kernel(n_col, far, m, meta, ids, *refs):
    pieces, (high, low) = refs[:n_col], refs[n_col : n_col + 2]
    outs, scratch = refs[n_col + 2 : n_col + 6], refs[n_col + 6]
    products(meta, pieces, high, low, scratch, n_col)
    breadth = scratch.shape[0]
    for arr in range(4):
        for place in range(2 * far + arr % 2):
            slot = jnp.maximum(ids[arr * 32 + place], 0)
            r = slot // breadth
            t = slot % breadth
            outs[arr][place * m : (place + 1) * m, :] = scratch[
                t, pl.ds(pl.multiple_of(r * m, 8), m), :
            ]


def finish_kernel(plan, slabs, meta, inverse, particle, *refs):
    ins, out, scratch = refs[:-2], refs[-2], refs[-1]
    breadth = scratch.shape[0]
    rows = scratch.shape[1]
    for s, first, entries in [(p[0], p[2], p[3]) for p in plan]:
        a, b = slabs[s]
        m = b - a
        for code, index, row in entries:
            tile = inverse[code]

            @pl.when(tile >= 0)
            def _(tile=tile, index=index, row=row, first=first, a=a, m=m):
                r = tile // breadth
                t = tile % breadth
                scratch[t, pl.ds(pl.multiple_of(r * TR + a, 8), m), :] = ins[first + index][
                    row : row + m, :
                ]

    size = meta[0]
    for r in range(0, rows, TR):
        for t in range(breadth):
            live = ((lax.broadcasted_iota(jnp.int32, (TR, TC), 0) + meta[1] + r) < size) & (
                (lax.broadcasted_iota(jnp.int32, (TR, TC), 1) + meta[2] + t * TC) < size
            )
            out[r : r + TR, t * TC : (t + 1) * TC] = jnp.where(
                live, particle[t, r : r + TR, :] - scratch[t, r : r + TR, :], 0.0
            )


def make_plan(streams):
    plan, first = [], 0
    for s, pair in enumerate(streams):
        for side, stream in enumerate(pair):
            arrays = stream.arrays
            entries = [(64 * side + c, i, row) for c, i, row, _ in stream.places()]
            plan.append((s, arrays, first, entries))
            first += len(arrays)
    return plan


def occupancy(orbit_pairs, occupations, size_limit, particle):
    orbit_ids = jnp.arange(occupations.shape[0], dtype=jnp.int32)
    filled = occupations.astype(F32)
    matches = (orbit_pairs[:, :, None] == orbit_ids[None, None, :]).astype(F32)
    looked_up = jnp.sum(matches * filled[None, None, :], axis=2)
    if particle:
        factor = 1.0 - looked_up[0] - looked_up[1]
    else:
        factor = looked_up[0] - looked_up[1]
    position_ids = jnp.arange(orbit_pairs.shape[1], dtype=jnp.int32)
    return (factor * (position_ids < size_limit).astype(F32))[:, None]


def panels(meta, block, w):
    other = lax.ppermute(block, "sub", [(0, 1), (1, 0)])
    rows, breadth = block.shape[2], block.shape[1]
    shape = jax.ShapeDtypeStruct((2, 2 * rows, breadth * TC), BF)
    return call(panel_kernel, [shape, shape], [meta, block, other, w], 1)


def across(x, n_col):
    return [x] + [send(x, "col", d, n_col) for d in range(1, n_col)]


def shards(
    generator,
    interaction,
    occupations,
    pair_orbits,
    cross_orbits,
    pair_sizes,
    cross_sizes,
    cross_target,
):
    rows, width = generator.shape[1:]
    breadth = width // TC
    n = lax.axis_size("chan")
    n_col = lax.axis_size("col")
    far = n // 4
    tile_count = rows // TR * breadth
    me, col, sub = lax.axis_index("chan"), lax.axis_index("col"), lax.axis_index("sub")
    meta = jnp.stack([pair_sizes[0], sub * rows, col * width, sub, col]).astype(jnp.int32)

    targets = cross_target[0].reshape(-1)
    owner = targets // tile_count
    same = owner[:, None] == owner[None, :]
    order = jnp.arange(tile_count, dtype=jnp.int32)
    rank = jnp.sum((same & (order[None, :] < order[:, None])).astype(jnp.int32), axis=1)
    ahead = jnp.remainder(owner - me, n)
    behind = n - ahead
    right = jnp.where(ahead < far, 2 * ahead, 32 + 2 * (ahead - far))
    left = jnp.where(behind < far, 64 + 2 * behind, 96 + 2 * (behind - far))
    half = jnp.where(rank == 0, 32 + 2 * far, 96 + 2 * far)
    codes = jnp.where(
        ahead < 2 * far, right + rank, jnp.where(ahead == 2 * far, half, left + rank)
    ).astype(jnp.int32)
    every = jnp.arange(128, dtype=jnp.int32)
    inverse = (
        jnp.sum(
            jnp.where(codes[None, :] == every[:, None], order[None, :] + 1, 0), axis=1
        ).astype(jnp.int32)
        - 1
    )

    outs = [f32(2, breadth, rows, TC)]
    widths = [b - a for a, b in FWD]
    for s, m in enumerate(widths):
        for arr in range(4):
            outs.append(
                f32(slot_rows(far, 2 * m, arr) + (id_rows(far, arr) if s == 0 else 0), TC)
            )
    packed = call(
        functools.partial(pack_kernel, far, FWD),
        outs,
        [codes, targets, meta, generator[0], interaction[0]],
        3,
    )
    live, packed = packed[0], packed[1:]
    groups = [packed[4 * s : 4 * s + 4] for s in range(len(FWD))]
    high, low = panels(meta, live, occupancy(pair_orbits[0], occupations, pair_sizes[0], True))
    particle = call(
        functools.partial(product_kernel, n_col),
        f32(breadth, rows, TC),
        [meta, *across(live, n_col), high, low],
        1,
    )
    streams, particle = transport(
        groups, [2 * m for m in widths], far, "chan", n, 1, True, particle
    )

    plan = make_plan(streams)
    first = len(streams[0][0].arrays)
    ids = call(
        functools.partial(
            ids_kernel,
            [
                (64 * side + c, first * side + i, id_row)
                for side, stream in enumerate(streams[0])
                for c, i, _, id_row in stream.places()
            ],
        ),
        jax.ShapeDtypeStruct((1, TC), jnp.int32),
        streams[0][0].arrays + streams[0][1].arrays,
        0,
        [pltpu.VMEM((TC, TC), F32)],
    ).reshape(TC)

    placed = call(
        functools.partial(place_kernel, plan, FWD, RET, breadth),
        [f32(2, breadth, rows, TC)]
        + [f32(2, breadth, rows // TR * (b - a), TC) for a, b in RET],
        [ids] + [a for p in plan for a in p[1]],
        1,
    )
    block, pieces = placed[0], placed[1:]
    high, low = panels(meta, block, occupancy(cross_orbits[0], occupations, cross_sizes[0], False))
    back = []
    for (a, b), piece in zip(RET, pieces):
        m = b - a
        if back:
            piece, back[-1][0] = lax.optimization_barrier((piece, back[-1][0]))
        back.append(
            call(
                functools.partial(product_pick_kernel, n_col, far, m),
                [f32(slot_rows(far, m, arr), TC) for arr in range(4)],
                [meta, ids, *across(piece, n_col), high, low],
                2,
                [pltpu.VMEM((breadth, rows // TR * m, TC), F32)],
            )
        )
        back[-1] = list(back[-1])
    streams, _ = transport(back, [b - a for a, b in RET], far, "chan", n, -1, False)
    plan = make_plan(streams)
    out = call(
        functools.partial(finish_kernel, plan, RET),
        f32(rows, width),
        [meta, inverse, particle] + [a for p in plan for a in p[1]],
        2,
        [pltpu.VMEM((breadth, rows, TC), F32)],
    )
    return out[None]


def solution(mesh):
    return jax.shard_map(
        shards,
        mesh=mesh,
        in_specs=(
            P(("grp", "chan"), "sub", "col"),
            P(("grp", "chan"), "sub", "col"),
            P(),
            P("chan", None, None),
            P("chan", None, None),
            P("chan"),
            P("chan"),
            P("chan", "sub", "col"),
        ),
        out_specs=P(("grp", "chan"), "sub", "col"),
        check_vma=False,
    )
```

```python
import functools

import jax
import jax.numpy as jnp
from jax import lax
from jax.experimental import pallas as pl
from jax.experimental.pallas import tpu as pltpu
from jax.sharding import PartitionSpec as P

TR = 32
TC = 128
BF = jnp.bfloat16
F32 = jnp.float32


def smem():
    return pl.BlockSpec(memory_space=pltpu.SMEM)


def vmem():
    return pl.BlockSpec(memory_space=pltpu.VMEM)


def call(kernel, out_shape, args, n_smem, scratch=()):
    flat_out = jax.tree.leaves(out_shape)
    return pl.pallas_call(
        kernel,
        out_shape=out_shape,
        in_specs=[smem()] * n_smem + [vmem()] * (len(args) - n_smem),
        out_specs=jax.tree.unflatten(jax.tree.structure(out_shape), [vmem()] * len(flat_out)),
        scratch_shapes=list(scratch),
        compiler_params=pltpu.CompilerParams(vmem_limit_bytes=48 * 1024 * 1024),
    )(*args)


def f32(*shape):
    return jax.ShapeDtypeStruct(shape, F32)


def pack_kernel(slots, meta, g_ref, h_ref, live_ref, out_ref):
    rows = g_ref.shape[0]
    breadth = g_ref.shape[1] // TC
    size = meta[0]
    row0 = meta[1]
    col0 = meta[2]

    def body(r, carry):
        at = pl.multiple_of(r * TR, TR)
        for t in range(breadth):
            slot = slots[r * breadth + t]
            live = ((lax.broadcasted_iota(jnp.int32, (TR, TC), 0) + row0 + r * TR) < size) & (
                (lax.broadcasted_iota(jnp.int32, (TR, TC), 1) + col0 + t * TC) < size
            )
            for mat, ref in enumerate((g_ref, h_ref)):
                x = jnp.where(live, ref[pl.ds(at, TR), t * TC : (t + 1) * TC], 0.0)
                live_ref[mat, t, pl.ds(at, TR), :] = x
                out_ref[slot // 2, slot % 2, mat * TR : (mat + 1) * TR, :] = x
        return carry

    lax.fori_loop(0, rows // TR, body, 0)


def send(x, axis, hop, n):
    return lax.ppermute(x, axis, [(i, (i + hop) % n) for i in range(n)])


def place_kernel(ids, got, block):
    breadth = block.shape[1]

    def body(peer, carry):
        for rank in range(2):
            tile = ids[2 * peer + rank]

            @pl.when(tile >= 0)
            def _(tile=tile, rank=rank):
                at = pl.ds(pl.multiple_of(tile // breadth * TR, TR), TR)
                for mat in range(2):
                    block[mat, tile % breadth, at, :] = got[
                        peer, rank, mat * TR : (mat + 1) * TR, :
                    ]

        return carry

    lax.fori_loop(0, got.shape[0], body, 0)


def halves(x):
    high = x.astype(BF)
    return high, (x - high.astype(F32)).astype(BF)


def panel_kernel(meta, own, other, w_ref, high, low):
    rows = own.shape[2]
    breadth = own.shape[1]
    mine = pl.multiple_of(meta[3] * rows, rows)
    theirs = pl.multiple_of((1 - meta[3]) * rows, rows)
    step = 128
    for src, base in ((own, mine), (other, theirs)):
        for k in range(0, rows, step):
            at = pl.ds(pl.multiple_of(base + k, step), step)
            w = w_ref[at, :]
            for mat in range(2):
                for t in range(breadth):
                    x = src[1 - mat, t, k : k + step, :] * w
                    if mat == 1:
                        x = -x
                    hi, lo = halves(x)
                    high[mat, at, t * TC : (t + 1) * TC] = hi
                    low[mat, at, t * TC : (t + 1) * TC] = lo


def products(meta, pieces, high, low, out, n_col):
    rows = pieces[0].shape[2]
    breadth = pieces[0].shape[1]
    width = breadth * TC
    step = 128
    for c in range(0, rows, step):
        acc = jnp.zeros((step, width), F32)
        for d in range(n_col):
            at = pl.ds(pl.multiple_of(lax.rem(meta[4] + n_col - d, n_col) * width, width), width)
            for mat in range(2):
                x = jnp.concatenate([pieces[d][mat, t, c : c + step, :] for t in range(breadth)], 1)
                hi, lo = halves(x)
                bh = high[mat, at, :]
                bl = low[mat, at, :]
                acc += jnp.dot(hi, bh, preferred_element_type=F32)
                acc += jnp.dot(hi, bl, preferred_element_type=F32)
                acc += jnp.dot(lo, bh, preferred_element_type=F32)
        for t in range(breadth):
            out[t, c : c + step, :] = acc[:, t * TC : (t + 1) * TC]


def product_kernel(n_col, meta, *refs):
    pieces, (high, low, out) = refs[:n_col], refs[n_col:]
    products(meta, pieces, high, low, out, n_col)


def product_pick_kernel(n_col, meta, ids, *refs):
    pieces, (high, low, out, scratch) = refs[:n_col], refs[n_col:]
    products(meta, pieces, high, low, scratch, n_col)
    breadth = scratch.shape[0]

    def body(peer, carry):
        for rank in range(2):
            tile = jnp.maximum(ids[2 * peer + rank], 0)
            at = pl.ds(pl.multiple_of(tile // breadth * TR, TR), TR)
            out[peer, rank] = scratch[tile % breadth, at, :]
        return carry

    lax.fori_loop(0, out.shape[0], body, 0)


def finish_kernel(meta, slots, particle, got, out):
    breadth = particle.shape[0]
    rows = particle.shape[1]
    size = meta[0]

    def body(r, carry):
        at = pl.multiple_of(r * TR, TR)
        for t in range(breadth):
            slot = slots[r * breadth + t]
            live = ((lax.broadcasted_iota(jnp.int32, (TR, TC), 0) + meta[1] + r * TR) < size) & (
                (lax.broadcasted_iota(jnp.int32, (TR, TC), 1) + meta[2] + t * TC) < size
            )
            out[pl.ds(at, TR), t * TC : (t + 1) * TC] = jnp.where(
                live, particle[t, pl.ds(at, TR), :] - got[slot // 2, slot % 2], 0.0
            )
        return carry

    lax.fori_loop(0, rows // TR, body, 0)


def occupancy(orbit_pairs, occupations, size_limit, particle):
    orbit_ids = jnp.arange(occupations.shape[0], dtype=jnp.int32)
    filled = occupations.astype(F32)
    matches = (orbit_pairs[:, :, None] == orbit_ids[None, None, :]).astype(F32)
    looked_up = jnp.sum(matches * filled[None, None, :], axis=2)
    if particle:
        factor = 1.0 - looked_up[0] - looked_up[1]
    else:
        factor = looked_up[0] - looked_up[1]
    position_ids = jnp.arange(orbit_pairs.shape[1], dtype=jnp.int32)
    return (factor * (position_ids < size_limit).astype(F32))[:, None]


def panels(meta, block, w):
    other = lax.ppermute(block, "sub", [(0, 1), (1, 0)])
    rows, breadth = block.shape[2], block.shape[1]
    shape = jax.ShapeDtypeStruct((2, 2 * rows, breadth * TC), BF)
    return call(panel_kernel, [shape, shape], [meta, block, other, w], 1)


def across(x, n_col):
    return [x] + [send(x, "col", d, n_col) for d in range(1, n_col)]


def shards(
    generator,
    interaction,
    occupations,
    pair_orbits,
    cross_orbits,
    pair_sizes,
    cross_sizes,
    cross_target,
):
    rows, width = generator.shape[1:]
    breadth = width // TC
    n = lax.axis_size("chan")
    n_col = lax.axis_size("col")
    tile_count = rows // TR * breadth
    me, col, sub = lax.axis_index("chan"), lax.axis_index("col"), lax.axis_index("sub")
    meta = jnp.stack([pair_sizes[0], sub * rows, col * width, sub, col]).astype(jnp.int32)

    targets = cross_target[0].reshape(-1)
    owner = targets // tile_count
    same = owner[:, None] == owner[None, :]
    order = jnp.arange(tile_count, dtype=jnp.int32)
    rank = jnp.sum((same & (order[None, :] < order[:, None])).astype(jnp.int32), axis=1)
    slots = (owner * 2 + rank).astype(jnp.int32)

    live, packed = call(
        pack_kernel,
        [f32(2, breadth, rows, TC), f32(n, 2, 2 * TR, TC)],
        [slots, meta, generator[0], interaction[0]],
        2,
    )
    got = lax.all_to_all(packed, "chan", split_axis=0, concat_axis=0, tiled=True)

    across_live = across(live, n_col)
    targets, across_live[-1] = lax.optimization_barrier((targets, across_live[-1]))
    table = lax.all_gather(targets, "chan")
    high, low = panels(meta, live, occupancy(pair_orbits[0], occupations, pair_sizes[0], True))
    particle = call(
        functools.partial(product_kernel, n_col),
        f32(breadth, rows, TC),
        [meta, *across_live, high, low],
        1,
    )
    mine = (table // tile_count == me).astype(jnp.int32)
    before = jnp.sum(
        mine[:, None, :] * (order[None, None, :] < order[None, :, None]).astype(jnp.int32), axis=2
    )
    each = jnp.arange(2, dtype=jnp.int32)
    ids = (
        jnp.sum(
            (mine * (table % tile_count + 1))[:, None, :]
            * (before[:, None, :] == each[None, :, None]).astype(jnp.int32),
            axis=2,
        ).astype(jnp.int32)
        - 1
    ).reshape(-1)

    block = call(place_kernel, f32(2, breadth, rows, TC), [ids, got], 1)
    high, low = panels(meta, block, occupancy(cross_orbits[0], occupations, cross_sizes[0], False))
    back = call(
        functools.partial(product_pick_kernel, n_col),
        f32(n, 2, TR, TC),
        [meta, ids, *across(block, n_col), high, low],
        2,
        [pltpu.VMEM((breadth, rows, TC), F32)],
    )
    returned = lax.all_to_all(back, "chan", split_axis=0, concat_axis=0, tiled=True)
    out = call(finish_kernel, f32(rows, width), [meta, slots, particle, returned], 2)
    return out[None]


def solution(mesh):
    return jax.shard_map(
        shards,
        mesh=mesh,
        in_specs=(
            P(("grp", "chan"), "sub", "col"),
            P(("grp", "chan"), "sub", "col"),
            P(),
            P("chan", None, None),
            P("chan", None, None),
            P("chan"),
            P("chan"),
            P("chan", "sub", "col"),
        ),
        out_specs=P(("grp", "chan"), "sub", "col"),
        check_vma=False,
    )
```

```python
import functools

import jax
import jax.numpy as jnp
from jax import lax
from jax.experimental import pallas as pl
from jax.experimental.pallas import tpu as pltpu
from jax.sharding import PartitionSpec as P

TR = 32
TC = 128
BF = jnp.bfloat16
F32 = jnp.float32


def smem():
    return pl.BlockSpec(memory_space=pltpu.SMEM)


def vmem():
    return pl.BlockSpec(memory_space=pltpu.VMEM)


def call(kernel, out_shape, args, n_smem, scratch=()):
    flat_out = jax.tree.leaves(out_shape)
    return pl.pallas_call(
        kernel,
        out_shape=out_shape,
        in_specs=[smem()] * n_smem + [vmem()] * (len(args) - n_smem),
        out_specs=jax.tree.unflatten(jax.tree.structure(out_shape), [vmem()] * len(flat_out)),
        scratch_shapes=list(scratch),
        compiler_params=pltpu.CompilerParams(vmem_limit_bytes=16 * 1024 * 1024),
    )(*args)


def f32(*shape):
    return jax.ShapeDtypeStruct(shape, F32)


def pack_kernel(slots, meta, g_ref, h_ref, live_ref, out_ref):
    rows = g_ref.shape[0]
    breadth = g_ref.shape[1] // TC
    size = meta[0]
    row0 = meta[1]
    col0 = meta[2]

    def body(r, carry):
        at = pl.multiple_of(r * TR, TR)
        for t in range(breadth):
            slot = slots[r * breadth + t]
            live = ((lax.broadcasted_iota(jnp.int32, (TR, TC), 0) + row0 + r * TR) < size) & (
                (lax.broadcasted_iota(jnp.int32, (TR, TC), 1) + col0 + t * TC) < size
            )
            for mat, ref in enumerate((g_ref, h_ref)):
                x = jnp.where(live, ref[pl.ds(at, TR), t * TC : (t + 1) * TC], 0.0)
                live_ref[mat, t, pl.ds(at, TR), :] = x
                out_ref[slot // 2, slot % 2, mat * TR : (mat + 1) * TR, :] = x
        return carry

    lax.fori_loop(0, rows // TR, body, 0)


def send(x, axis, hop, n):
    return lax.ppermute(x, axis, [(i, (i + hop) % n) for i in range(n)])


def place_kernel(ids, got, block):
    breadth = block.shape[1]

    def body(peer, carry):
        for rank in range(2):
            tile = ids[2 * peer + rank]

            @pl.when(tile >= 0)
            def _(tile=tile, rank=rank):
                at = pl.ds(pl.multiple_of(tile // breadth * TR, TR), TR)
                for mat in range(2):
                    block[mat, tile % breadth, at, :] = got[
                        peer, rank, mat * TR : (mat + 1) * TR, :
                    ]

        return carry

    lax.fori_loop(0, got.shape[0], body, 0)


def halves(x):
    high = x.astype(BF)
    return high, (x - high.astype(F32)).astype(BF)


def panel_kernel(meta, own, other, w_ref, high, low):
    rows = own.shape[2]
    breadth = own.shape[1]
    mine = pl.multiple_of(meta[3] * rows, rows)
    theirs = pl.multiple_of((1 - meta[3]) * rows, rows)
    step = 128
    for src, base in ((own, mine), (other, theirs)):
        for k in range(0, rows, step):
            at = pl.ds(pl.multiple_of(base + k, step), step)
            w = w_ref[at, :]
            for mat in range(2):
                for t in range(breadth):
                    x = src[1 - mat, t, k : k + step, :] * w
                    if mat == 1:
                        x = -x
                    hi, lo = halves(x)
                    high[mat, at, t * TC : (t + 1) * TC] = hi
                    low[mat, at, t * TC : (t + 1) * TC] = lo


def products(meta, pieces, hops, high, low, start, out, n_col):
    rows = pieces[0].shape[2]
    breadth = pieces[0].shape[1]
    width = breadth * TC
    step = 128
    for c in range(0, rows, step):
        if start is None:
            acc = jnp.zeros((step, width), F32)
        else:
            acc = jnp.concatenate([start[t, c : c + step, :] for t in range(breadth)], 1)
        for piece, d in zip(pieces, hops):
            at = pl.ds(pl.multiple_of(lax.rem(meta[4] + n_col - d, n_col) * width, width), width)
            for mat in range(2):
                x = jnp.concatenate([piece[mat, t, c : c + step, :] for t in range(breadth)], 1)
                hi, lo = halves(x)
                bh = high[mat, at, :]
                bl = low[mat, at, :]
                acc += jnp.dot(hi, bh, preferred_element_type=F32)
                acc += jnp.dot(hi, bl, preferred_element_type=F32)
                acc += jnp.dot(lo, bh, preferred_element_type=F32)
        for t in range(breadth):
            out[t, c : c + step, :] = acc[:, t * TC : (t + 1) * TC]


def product_kernel(n_col, hops, meta, *refs):
    pieces, (high, low, out) = refs[: len(hops)], refs[len(hops) :]
    products(meta, pieces, hops, high, low, None, out, n_col)


def product_pick_kernel(n_col, hops, meta, ids, *refs):
    pieces, (high, low, start, out, scratch) = refs[: len(hops)], refs[len(hops) :]
    products(meta, pieces, hops, high, low, start, scratch, n_col)
    breadth = scratch.shape[0]

    def body(peer, carry):
        for rank in range(2):
            tile = jnp.maximum(ids[2 * peer + rank], 0)
            at = pl.ds(pl.multiple_of(tile // breadth * TR, TR), TR)
            out[peer, rank] = scratch[tile % breadth, at, :]
        return carry

    lax.fori_loop(0, out.shape[0], body, 0)


def finish_kernel(meta, slots, particle, got, out):
    breadth = particle.shape[0]
    rows = particle.shape[1]
    size = meta[0]

    def body(r, carry):
        at = pl.multiple_of(r * TR, TR)
        for t in range(breadth):
            slot = slots[r * breadth + t]
            live = ((lax.broadcasted_iota(jnp.int32, (TR, TC), 0) + meta[1] + r * TR) < size) & (
                (lax.broadcasted_iota(jnp.int32, (TR, TC), 1) + meta[2] + t * TC) < size
            )
            out[pl.ds(at, TR), t * TC : (t + 1) * TC] = jnp.where(
                live, particle[t, pl.ds(at, TR), :] - got[slot // 2, slot % 2], 0.0
            )
        return carry

    lax.fori_loop(0, rows // TR, body, 0)


def occupancy(orbit_pairs, occupations, size_limit, particle):
    orbit_ids = jnp.arange(occupations.shape[0], dtype=jnp.int32)
    filled = occupations.astype(F32)
    matches = (orbit_pairs[:, :, None] == orbit_ids[None, None, :]).astype(F32)
    looked_up = jnp.sum(matches * filled[None, None, :], axis=2)
    if particle:
        factor = 1.0 - looked_up[0] - looked_up[1]
    else:
        factor = looked_up[0] - looked_up[1]
    position_ids = jnp.arange(orbit_pairs.shape[1], dtype=jnp.int32)
    return (factor * (position_ids < size_limit).astype(F32))[:, None]


def panels(meta, block, w):
    other = lax.ppermute(block, "sub", [(0, 1), (1, 0)])
    rows, breadth = block.shape[2], block.shape[1]
    shape = jax.ShapeDtypeStruct((2, 2 * rows, breadth * TC), BF)
    return call(panel_kernel, [shape, shape], [meta, block, other, w], 1)


def across(x, n_col):
    return [x] + [send(x, "col", d, n_col) for d in range(1, n_col)]


def shards(
    generator,
    interaction,
    occupations,
    pair_orbits,
    cross_orbits,
    pair_sizes,
    cross_sizes,
    cross_target,
):
    rows, width = generator.shape[1:]
    breadth = width // TC
    n = lax.axis_size("chan")
    n_col = lax.axis_size("col")
    tile_count = rows // TR * breadth
    me, col, sub = lax.axis_index("chan"), lax.axis_index("col"), lax.axis_index("sub")
    meta = jnp.stack([pair_sizes[0], sub * rows, col * width, sub, col]).astype(jnp.int32)

    targets = cross_target[0].reshape(-1)
    owner = targets // tile_count
    same = owner[:, None] == owner[None, :]
    order = jnp.arange(tile_count, dtype=jnp.int32)
    rank = jnp.sum((same & (order[None, :] < order[:, None])).astype(jnp.int32), axis=1)
    slots = (owner * 2 + rank).astype(jnp.int32)

    live, packed = call(
        pack_kernel,
        [f32(2, breadth, rows, TC), f32(n, 2, 2 * TR, TC)],
        [slots, meta, generator[0], interaction[0]],
        2,
    )
    got = lax.all_to_all(packed, "chan", split_axis=0, concat_axis=0, tiled=True)

    weights = (
        occupancy(pair_orbits[0], occupations, pair_sizes[0], True),
        occupancy(cross_orbits[0], occupations, cross_sizes[0], False),
    )
    live, weights = lax.optimization_barrier((live, weights))
    high, low = panels(meta, live, weights[0])
    particle = call(
        functools.partial(product_kernel, n_col, tuple(range(n_col))),
        f32(breadth, rows, TC),
        [meta, *across(live, n_col), high, low],
        1,
    )
    targets, particle, cross_weight = lax.optimization_barrier((targets, particle, weights[1]))
    table = lax.all_gather(targets, "chan")
    mine = (table // tile_count == me).astype(jnp.int32)
    before = jnp.sum(
        mine[:, None, :] * (order[None, None, :] < order[None, :, None]).astype(jnp.int32), axis=2
    )
    each = jnp.arange(2, dtype=jnp.int32)
    ids = (
        jnp.sum(
            (mine * (table % tile_count + 1))[:, None, :]
            * (before[:, None, :] == each[None, :, None]).astype(jnp.int32),
            axis=2,
        ).astype(jnp.int32)
        - 1
    ).reshape(-1)

    block = call(place_kernel, f32(2, breadth, rows, TC), [ids, got], 1)
    high, low = panels(meta, block, cross_weight)
    pieces = across(block, n_col)
    late = n_col // 2
    hops = [d for d in range(n_col) if d != late]
    part = call(
        functools.partial(product_kernel, n_col, hops),
        f32(breadth, rows, TC),
        [meta, *[pieces[d] for d in hops], high, low],
        1,
    )
    back = call(
        functools.partial(product_pick_kernel, n_col, [late]),
        f32(n, 2, TR, TC),
        [meta, ids, pieces[late], high, low, part],
        2,
        [pltpu.VMEM((breadth, rows, TC), F32)],
    )
    returned = lax.all_to_all(back, "chan", split_axis=0, concat_axis=0, tiled=True)
    out = call(finish_kernel, f32(rows, width), [meta, slots, particle, returned], 2)
    return out[None]


def solution(mesh):
    return jax.shard_map(
        shards,
        mesh=mesh,
        in_specs=(
            P(("grp", "chan"), "sub", "col"),
            P(("grp", "chan"), "sub", "col"),
            P(),
            P("chan", None, None),
            P("chan", None, None),
            P("chan"),
            P("chan"),
            P("chan", "sub", "col"),
        ),
        out_specs=P(("grp", "chan"), "sub", "col"),
        check_vma=False,
    )
```

```python
import functools

import jax
import jax.numpy as jnp
from jax import lax
from jax.experimental import pallas as pl
from jax.experimental.pallas import tpu as pltpu
from jax.sharding import PartitionSpec as P

TR = 32
TC = 128
BF = jnp.bfloat16
F32 = jnp.float32


def smem():
    return pl.BlockSpec(memory_space=pltpu.SMEM)


def vmem():
    return pl.BlockSpec(memory_space=pltpu.VMEM)


def call(kernel, out_shape, args, n_smem, scratch=()):
    flat_out = jax.tree.leaves(out_shape)
    return pl.pallas_call(
        kernel,
        out_shape=out_shape,
        in_specs=[smem()] * n_smem + [vmem()] * (len(args) - n_smem),
        out_specs=jax.tree.unflatten(jax.tree.structure(out_shape), [vmem()] * len(flat_out)),
        scratch_shapes=list(scratch),
        compiler_params=pltpu.CompilerParams(vmem_limit_bytes=16 * 1024 * 1024),
    )(*args)


def f32(*shape):
    return jax.ShapeDtypeStruct(shape, F32)


def pack_kernel(slots, meta, g_ref, h_ref, live_g, live_h, out_ref):
    rows = g_ref.shape[0]
    breadth = g_ref.shape[1] // TC
    size = meta[0]
    row0 = meta[1]
    col0 = meta[2]

    def body(r, carry):
        at = pl.multiple_of(r * TR, TR)
        for t in range(breadth):
            slot = slots[r * breadth + t]
            live = ((lax.broadcasted_iota(jnp.int32, (TR, TC), 0) + row0 + r * TR) < size) & (
                (lax.broadcasted_iota(jnp.int32, (TR, TC), 1) + col0 + t * TC) < size
            )
            for mat, (ref, live_ref) in enumerate(((g_ref, live_g), (h_ref, live_h))):
                x = jnp.where(live, ref[pl.ds(at, TR), t * TC : (t + 1) * TC], 0.0)
                live_ref[t, pl.ds(at, TR), :] = x
                out_ref[slot // 2, slot % 2, mat * TR : (mat + 1) * TR, :] = x
        return carry

    lax.fori_loop(0, rows // TR, body, 0)


def send(x, axis, hop, n):
    return lax.ppermute(x, axis, [(i, (i + hop) % n) for i in range(n)])


def place_kernel(ids, got, *block):
    breadth = block[0].shape[0]

    def body(peer, carry):
        for rank in range(2):
            tile = ids[2 * peer + rank]

            @pl.when(tile >= 0)
            def _(tile=tile, rank=rank):
                at = pl.ds(pl.multiple_of(tile // breadth * TR, TR), TR)
                for mat in range(2):
                    block[mat][tile % breadth, at, :] = got[
                        peer, rank, mat * TR : (mat + 1) * TR, :
                    ]

        return carry

    lax.fori_loop(0, got.shape[0], body, 0)


def halves(x):
    high = x.astype(BF)
    return high, (x - high.astype(F32)).astype(BF)


def panel_kernel(meta, own_g, own_h, other_g, other_h, w_ref, high, low):
    breadth, rows = own_g.shape[:2]
    mine = pl.multiple_of(meta[3] * rows, rows)
    theirs = pl.multiple_of((1 - meta[3]) * rows, rows)
    step = 128
    for src, base in (((own_g, own_h), mine), ((other_g, other_h), theirs)):
        for k in range(0, rows, step):
            at = pl.ds(pl.multiple_of(base + k, step), step)
            w = w_ref[at, :]
            for mat in range(2):
                for t in range(breadth):
                    x = src[1 - mat][t, k : k + step, :] * w
                    if mat == 1:
                        x = -x
                    hi, lo = halves(x)
                    high[mat, at, t * TC : (t + 1) * TC] = hi
                    low[mat, at, t * TC : (t + 1) * TC] = lo


def products(meta, pieces, hops, high, low, start, out, n_col):
    breadth, rows = pieces[0].shape[:2]
    width = breadth * TC
    step = 128
    for c in range(0, rows, step):
        if start is None:
            acc = jnp.zeros((step, width), F32)
        else:
            acc = jnp.concatenate([start[t, c : c + step, :] for t in range(breadth)], 1)
        for k, d in enumerate(hops):
            at = pl.ds(pl.multiple_of(lax.rem(meta[4] + n_col - d, n_col) * width, width), width)
            for mat in range(2):
                piece = pieces[2 * k + mat]
                x = jnp.concatenate([piece[t, c : c + step, :] for t in range(breadth)], 1)
                hi, lo = halves(x)
                bh = high[mat, at, :]
                bl = low[mat, at, :]
                acc += jnp.dot(hi, bh, preferred_element_type=F32)
                acc += jnp.dot(hi, bl, preferred_element_type=F32)
                acc += jnp.dot(lo, bh, preferred_element_type=F32)
        for t in range(breadth):
            out[t, c : c + step, :] = acc[:, t * TC : (t + 1) * TC]


def product_kernel(n_col, hops, meta, *refs):
    pieces, (high, low, out) = refs[: 2 * len(hops)], refs[2 * len(hops) :]
    products(meta, pieces, hops, high, low, None, out, n_col)


def product_pick_kernel(n_col, hops, meta, ids, *refs):
    pieces, (high, low, start, out, scratch) = refs[: 2 * len(hops)], refs[2 * len(hops) :]
    products(meta, pieces, hops, high, low, start, scratch, n_col)
    breadth = scratch.shape[0]

    def body(peer, carry):
        for rank in range(2):
            tile = jnp.maximum(ids[2 * peer + rank], 0)
            at = pl.ds(pl.multiple_of(tile // breadth * TR, TR), TR)
            out[peer, rank] = scratch[tile % breadth, at, :]
        return carry

    lax.fori_loop(0, out.shape[0], body, 0)


def finish_kernel(meta, slots, particle, got, out):
    breadth = particle.shape[0]
    rows = particle.shape[1]
    size = meta[0]

    def body(r, carry):
        at = pl.multiple_of(r * TR, TR)
        for t in range(breadth):
            slot = slots[r * breadth + t]
            live = ((lax.broadcasted_iota(jnp.int32, (TR, TC), 0) + meta[1] + r * TR) < size) & (
                (lax.broadcasted_iota(jnp.int32, (TR, TC), 1) + meta[2] + t * TC) < size
            )
            out[pl.ds(at, TR), t * TC : (t + 1) * TC] = jnp.where(
                live, particle[t, pl.ds(at, TR), :] - got[slot // 2, slot % 2], 0.0
            )
        return carry

    lax.fori_loop(0, rows // TR, body, 0)


def occupancy(orbit_pairs, occupations, size_limit, particle):
    orbit_ids = jnp.arange(occupations.shape[0], dtype=jnp.int32)
    filled = occupations.astype(F32)
    matches = (orbit_pairs[:, :, None] == orbit_ids[None, None, :]).astype(F32)
    looked_up = jnp.sum(matches * filled[None, None, :], axis=2)
    if particle:
        factor = 1.0 - looked_up[0] - looked_up[1]
    else:
        factor = looked_up[0] - looked_up[1]
    position_ids = jnp.arange(orbit_pairs.shape[1], dtype=jnp.int32)
    return (factor * (position_ids < size_limit).astype(F32))[:, None]


def panels(meta, block, w):
    other = [lax.ppermute(x, "sub", [(0, 1), (1, 0)]) for x in block]
    breadth, rows = block[0].shape[:2]
    shape = jax.ShapeDtypeStruct((2, 2 * rows, breadth * TC), BF)
    return call(panel_kernel, [shape, shape], [meta, *block, *other, w], 1)


def across(block, n_col):
    g, h = block
    from_left_g = send(g, "col", 1, n_col)
    from_right_h = send(h, "col", -1, n_col)
    from_left_h = send(h, "col", 1, n_col)
    from_right_g = send(g, "col", -1, n_col)
    far_g = send(from_left_g, "col", 1, n_col)
    far_h = send(from_right_h, "col", -1, n_col)
    return [(g, h), (from_left_g, from_left_h), (far_g, far_h), (from_right_g, from_right_h)]


def flat(pairs):
    return [x for pair in pairs for x in pair]


def shards(
    generator,
    interaction,
    occupations,
    pair_orbits,
    cross_orbits,
    pair_sizes,
    cross_sizes,
    cross_target,
):
    rows, width = generator.shape[1:]
    breadth = width // TC
    n = lax.axis_size("chan")
    n_col = lax.axis_size("col")
    tile_count = rows // TR * breadth
    me, col, sub = lax.axis_index("chan"), lax.axis_index("col"), lax.axis_index("sub")
    meta = jnp.stack([pair_sizes[0], sub * rows, col * width, sub, col]).astype(jnp.int32)

    targets = cross_target[0].reshape(-1)
    owner = targets // tile_count
    same = owner[:, None] == owner[None, :]
    order = jnp.arange(tile_count, dtype=jnp.int32)
    rank = jnp.sum((same & (order[None, :] < order[:, None])).astype(jnp.int32), axis=1)
    slots = (owner * 2 + rank).astype(jnp.int32)

    one = f32(breadth, rows, TC)
    *live, packed = call(
        pack_kernel,
        [one, one, f32(n, 2, 2 * TR, TC)],
        [slots, meta, generator[0], interaction[0]],
        2,
    )
    got = lax.all_to_all(packed, "chan", split_axis=0, concat_axis=0, tiled=True)

    weights = (
        occupancy(pair_orbits[0], occupations, pair_sizes[0], True),
        occupancy(cross_orbits[0], occupations, cross_sizes[0], False),
    )
    live, weights = lax.optimization_barrier((live, weights))
    high, low = panels(meta, live, weights[0])
    particle = call(
        functools.partial(product_kernel, n_col, tuple(range(n_col))),
        f32(breadth, rows, TC),
        [meta, *flat(across(live, n_col)), high, low],
        1,
    )
    targets, particle, cross_weight = lax.optimization_barrier((targets, particle, weights[1]))
    table = lax.all_gather(targets, "chan")
    mine = (table // tile_count == me).astype(jnp.int32)
    before = jnp.sum(
        mine[:, None, :] * (order[None, None, :] < order[None, :, None]).astype(jnp.int32), axis=2
    )
    each = jnp.arange(2, dtype=jnp.int32)
    ids = (
        jnp.sum(
            (mine * (table % tile_count + 1))[:, None, :]
            * (before[:, None, :] == each[None, :, None]).astype(jnp.int32),
            axis=2,
        ).astype(jnp.int32)
        - 1
    ).reshape(-1)

    block = call(place_kernel, [one, one], [ids, got], 1)
    high, low = panels(meta, block, cross_weight)
    pieces = across(block, n_col)
    late = n_col // 2
    hops = [d for d in range(n_col) if d != late]
    part = call(
        functools.partial(product_kernel, n_col, hops),
        f32(breadth, rows, TC),
        [meta, *flat(pieces[d] for d in hops), high, low],
        1,
    )
    back = call(
        functools.partial(product_pick_kernel, n_col, [late]),
        f32(n, 2, TR, TC),
        [meta, ids, *pieces[late], high, low, part],
        2,
        [pltpu.VMEM((breadth, rows, TC), F32)],
    )
    returned = lax.all_to_all(back, "chan", split_axis=0, concat_axis=0, tiled=True)
    out = call(finish_kernel, f32(rows, width), [meta, slots, particle, returned], 2)
    return out[None]


def solution(mesh):
    return jax.shard_map(
        shards,
        mesh=mesh,
        in_specs=(
            P(("grp", "chan"), "sub", "col"),
            P(("grp", "chan"), "sub", "col"),
            P(),
            P("chan", None, None),
            P("chan", None, None),
            P("chan"),
            P("chan"),
            P("chan", "sub", "col"),
        ),
        out_specs=P(("grp", "chan"), "sub", "col"),
        check_vma=False,
    )
```
